32 devices in a mesh: lat: 4 (over y, x), lon: 8 (over z, core).
Axes of the slice: x: 2, y: 2, z: 4, core: 2. Of those that a mesh axis runs over, the one named last changes fastest.
Arguments:
- transport: bfloat16 [48, 512, 3072], P(None, 'lat', 'lon'), may hold values from -0.0625 to 0.0625
- sigma_class: int32 [48, 512, 3072], P(None, 'lat', 'lon'), may hold values from 0 to 199
- basin_id: int32 [512, 3072], P('lat', 'lon'), may hold values from 0 to 3
- depth_levels: int32 [512, 3072], P('lat', 'lon'), may hold values from 0 to 48
Outputs:
- overturning: bfloat16 [4, 200, 512], replicated
The draws below stay inside these ranges and needn't reach their ends.
Inputs may be any that keep to these rules, and one draw needn't show every extreme that they name: `depth_levels`: 0 marks a land column.
All inputs are finite; a program needn't handle non-finite values.
Results may differ from the reference program's by a relative error of at most 0.001.
Values may be sent and summed in bfloat16 or wider, within the bound.
A program may use at most 64 MiB of HBM per device.

```python
import jax
import jax.numpy as jnp
from jax import lax

CLASSES = 200
BASINS = 4
ROWS_DEV = 128
COLS_DEV = 384
LEVELS = 48
NJ = 512
NI = 3072
N_LON = 8


def touch_ends(values, own_key, low, high):
    longest = values.shape.index(max(values.shape))
    spots = []
    for shift in (0, 1):
        where = [jax.random.randint(jax.random.fold_in(own_key, axis), (), 0, length) for axis, length in enumerate(values.shape)]
        where[longest] = (where[longest] + shift) % values.shape[longest]
        spots.append(tuple(where))
    return values.at[spots[0]].set(low).at[spots[1]].set(high)


def steps_of(key, dims, cuts, low, largest):
    def one(dim, shards_of):
        draws = jax.random.uniform(jax.random.fold_in(jax.random.fold_in(key, 6), dim), (shards_of,), jnp.float32, low / len(cuts), largest / len(cuts))
        return jnp.repeat(jnp.exp(draws), dims[dim] // shards_of).reshape((-1,) + (1,) * (len(dims) - dim - 1))

    factor_of = one(*cuts[0])
    for cut in cuts[1:]:
        factor_of = factor_of * one(*cut)
    return factor_of


def bell_draw(key, extent, deviation, reach, split=(), held_as=jnp.bfloat16):
    result = jax.random.normal(key, extent, jnp.float32) * deviation
    if len(split) > 0:
        result = steps_of(key, extent, split, -0.22, 0.18) * result
    return jnp.clip(result, min=-reach, max=reach).astype(held_as)


def setup_inputs(seed: int = 0) -> dict:
    key_of = jax.random.split(jax.random.key(seed), 5)
    return {
        "transport": bell_draw(key_of[0], (LEVELS, NJ, NI), (2.0 / (COLS_DEV * N_LON * LEVELS / BASINS) ** 0.5), 0.0625, ((1, 4), (2, 8))),
        "sigma_class": touch_ends(jax.random.randint(key_of[1], (LEVELS, NJ, NI), 0, CLASSES), jax.random.fold_in(key_of[1], 1), 0, CLASSES - 1).astype(jnp.int32),
        "basin_id": touch_ends(jax.random.randint(key_of[2], (NJ, NI), 0, BASINS), jax.random.fold_in(key_of[2], 1), 0, BASINS - 1).astype(jnp.int32),
        "depth_levels": touch_ends(jax.random.randint(key_of[3], (NJ, NI), 0, LEVELS + 1), jax.random.fold_in(key_of[3], 1), 0, LEVELS).astype(jnp.int32),
    }


def bin_block(transport, sigma_class, basin_id, depth_levels):
    depth_count, row_count, col_count = sigma_class.shape
    level_index = lax.broadcasted_iota(jnp.int32, (depth_count, row_count, col_count), 0)
    row_index = lax.broadcasted_iota(jnp.int32, (depth_count, row_count, col_count), 1)
    wet_cells = level_index < depth_levels[None, :, :]
    weights = jnp.where(wet_cells, transport.astype(jnp.float32), jnp.float32(0.0))
    bin_index = ((basin_id[None, :, :] * CLASSES + sigma_class) * row_count + row_index).astype(jnp.int32)
    flat = jax.ops.segment_sum(weights.reshape(-1), bin_index.reshape(-1), num_segments=BASINS * CLASSES * row_count)
    return flat.reshape(BASINS, CLASSES, row_count)


def reference(transport, sigma_class, basin_id, depth_levels):
    block_count = NJ // ROWS_DEV

    def one_block(start):
        return bin_block(
            lax.dynamic_slice_in_dim(transport, start, ROWS_DEV, 1),
            lax.dynamic_slice_in_dim(sigma_class, start, ROWS_DEV, 1),
            lax.dynamic_slice_in_dim(basin_id, start, ROWS_DEV, 0),
            lax.dynamic_slice_in_dim(depth_levels, start, ROWS_DEV, 0),
        )

    starts = (jnp.arange(block_count) * ROWS_DEV).astype(jnp.int32)
    tables = lax.map(one_block, starts)
    table = jnp.transpose(tables, (1, 2, 0, 3)).reshape(BASINS, CLASSES, NJ)
    return jnp.cumsum(table, axis=1).astype(jnp.bfloat16)
```

```python
import functools

import jax
import jax.numpy as jnp
import numpy as np
from jax import lax
from jax.experimental import pallas as pl
from jax.experimental.pallas import tpu as pltpu
from jax.sharding import PartitionSpec as P

CLASSES = 200
BASINS = 4
SUB = 8
LANES = 128
TILE = 256
STEP_ROWS = 16
MESH = pl.DeviceIdType.MESH
HIGHS = 26
HIGH_BLOCKS = 4


def hot_pairs(index, count, value):
    return [jnp.where(index == jnp.bfloat16(2 * i), value, jnp.bfloat16(0)) for i in range(count)]


def doubled(index):
    pair = jnp.concatenate([index, index - 1], axis=0)
    return pair.astype(jnp.float32).astype(jnp.bfloat16)


def squeeze_rows(product):
    rows = lax.broadcasted_iota(jnp.int32, (SUB, TILE), 0)
    lanes = lax.broadcasted_iota(jnp.int32, (SUB, TILE), 1)
    own = (lanes % SUB) == rows
    blocks = []
    for q in range(HIGH_BLOCKS):
        total = None
        for s in range(SUB):
            high = q * SUB + s
            if high * SUB >= CLASSES:
                break
            piece = jnp.where(own, product[high * SUB:(high + 1) * SUB, :], 0.0)
            piece = piece if s == 0 else pltpu.roll(piece, s, 1)
            total = piece if total is None else total + piece
        straight = jnp.where(rows == 0, total, 0.0)
        for r in range(1, SUB):
            straight = jnp.where(rows == r, pltpu.roll(total, TILE - r, 1), straight)
        blocks.append(straight)
    return jnp.concatenate(blocks, axis=1)


def bin_kernel(flow_ref, class_ref, basin_ref, depth_ref, out_ref, acc_ref):
    levels, _, cols = class_ref.shape
    chunks = cols // LANES
    per_trip = 4
    for half in range(STEP_ROWS // SUB):
        rows = slice(half * SUB, (half + 1) * SUB)

        def trip(t, carry, rows=rows):
            tiles = []
            for u in range(per_trip):
                level = t * per_trip + u
                for c in range(chunks):
                    lanes = slice(c * LANES, (c + 1) * LANES)
                    klass = class_ref[level, rows, lanes]
                    flow = flow_ref[level, :, lanes].astype(jnp.float32)[rows]
                    flow = jnp.where(level < depth_ref[rows, lanes], flow, 0.0)
                    high = doubled(klass >> 3)
                    low = doubled(basin_ref[rows, lanes] * SUB + (klass & 7))
                    value = jnp.concatenate([flow, flow], axis=0).astype(jnp.bfloat16)
                    tiles.append((
                        jnp.concatenate(hot_pairs(high, HIGHS // 2, value), axis=0),
                        jnp.concatenate(hot_pairs(low, TILE // (2 * SUB), jnp.bfloat16(1)), axis=0),
                    ))
            left = jnp.concatenate([x for x, _ in tiles], axis=1)
            right = jnp.concatenate([y for _, y in tiles], axis=1)
            acc_ref[...] += lax.dot_general(
                left, right, (((1,), (1,)), ((), ())), preferred_element_type=jnp.float32
            )
            return carry

        acc_ref[...] = jnp.zeros_like(acc_ref)
        lax.fori_loop(0, levels // per_trip, trip, 0)
        product = acc_ref[...]
        out_ref[rows, :] = squeeze_rows(product)


def bin_rows(transport, sigma_class, basin_id, depth_levels):
    levels, row_count, cols = sigma_class.shape
    deep = pl.BlockSpec((levels, STEP_ROWS, cols), lambda i: (0, i, 0))
    flat = pl.BlockSpec((STEP_ROWS, cols), lambda i: (i, 0))
    width = HIGH_BLOCKS * TILE
    return pl.pallas_call(
        bin_kernel,
        grid=(row_count // STEP_ROWS,),
        in_specs=[deep, deep, flat, flat],
        out_specs=pl.BlockSpec((STEP_ROWS, width), lambda i: (i, 0)),
        out_shape=jax.ShapeDtypeStruct((row_count, width), jnp.float32),
        scratch_shapes=[pltpu.VMEM((HIGHS * SUB, TILE), jnp.float32)],
        name="bin_rows",
    )(transport, sigma_class, basin_id, depth_levels)


def running_sums():
    row = np.arange(HIGH_BLOCKS * LANES)
    column = np.arange(2 * TILE)
    lane = row % LANES
    klass = (row // LANES) * 64 + (lane % SUB) * SUB + (lane % 64) // SUB
    same = (lane // 64)[:, None] == (column // TILE)[None, :]
    return (same & (klass[:, None] <= (column % TILE)[None, :])).astype(jnp.bfloat16)


def accumulate(share, sums):
    pieces = []
    for pair in range(BASINS // 2):
        lanes = [share[:, q * TILE + pair * LANES:q * TILE + (pair + 1) * LANES] for q in range(HIGH_BLOCKS)]
        rest = jnp.concatenate(lanes, axis=1)
        total = None
        for _ in range(3):
            part = rest.astype(jnp.bfloat16)
            rest = rest - part.astype(jnp.float32)
            term = jnp.dot(part, sums, preferred_element_type=jnp.float32)
            total = term if total is None else total + term
        pieces.append(total)
    return jnp.concatenate(pieces, axis=1)


def share_kernel(lats, lons, table_ref, sums_ref, out_ref, half, acc, arrived, sums, sum_sem,
                 half_send, half_recv, arr_send, arr_recv, out_send, out_recv):
    lat, lon = lax.axis_index("lat"), lax.axis_index("lon")
    zs = lons // 2
    z, core = lon // 2, lax.rem(lon, 2)
    partner = (lat, z * 2 + (1 - core))
    z_peers = [(lat, lax.rem(z + k, zs) * 2 + core) for k in range(1, zs)]
    lat_peers = [(lax.rem(lat + k, lats), lon) for k in range(1, lats)]

    load = pltpu.make_async_copy(sums_ref, sums, sum_sem)
    load.start()
    barrier = pltpu.get_barrier_semaphore()
    everyone = [partner] + z_peers + lat_peers
    for peer in everyone:
        pl.semaphore_signal(barrier, inc=1, device_id=peer, device_id_type=MESH)
    pl.semaphore_wait(barrier, len(everyone))

    def send(src, dst, send_sem, recv_sem, peer):
        copy = pltpu.make_async_remote_copy(
            src_ref=src, dst_ref=dst, send_sem=send_sem, recv_sem=recv_sem,
            device_id=peer, device_id_type=MESH,
        )
        copy.start()
        return copy

    swaps = []
    for k in [*range(1, zs), 0]:
        d = lax.rem(z + k, zs)
        swaps.append((k, send(table_ref.at[2 * d + (1 - core)], half.at[k], half_send.at[k], half_recv.at[k], partner)))
    moves = []
    for k, swap in swaps:
        swap.wait_recv()
        d = lax.rem(z + k, zs)
        acc[k] = table_ref[2 * d + core] + half[k]
        if k > 0:
            moves.append(send(acc.at[k], arrived.at[k - 1], arr_send.at[k - 1], arr_recv.at[k - 1], z_peers[k - 1]))
    share = acc[0]
    for k in range(1, zs):
        moves[k - 1].wait_recv()
        share = share + arrived[k - 1]
    load.wait()
    me = lat * lons + lon
    out_ref[me] = accumulate(share, sums[...]).astype(jnp.bfloat16)

    copies = []

    def spread(owner, peer):
        n = len(copies)
        copies.append(send(out_ref.at[owner], out_ref.at[owner], out_send.at[n], out_recv.at[owner], peer))

    def landed(owner):
        pltpu.make_async_remote_copy(
            src_ref=out_ref.at[owner], dst_ref=out_ref.at[owner], send_sem=out_send.at[0],
            recv_sem=out_recv.at[owner], device_id=partner, device_id_type=MESH,
        ).wait_recv()

    for peer in z_peers + lat_peers:
        spread(me, peer)
    spread(me, partner)
    for k in range(1, zs):
        owner = lat * lons + lax.rem(z - k + zs, zs) * 2 + core
        landed(owner)
        for peer in lat_peers + [partner]:
            spread(owner, peer)
    for j in range(zs):
        for k in range(1, lats):
            owner = lax.rem(lat - k + lats, lats) * lons + lax.rem(z - j + zs, zs) * 2 + core
            landed(owner)
            spread(owner, partner)
    for j in range(zs):
        for k in range(lats):
            landed(lax.rem(lat - k + lats, lats) * lons + lax.rem(z - j + zs, zs) * 2 + (1 - core))
    for _, swap in swaps:
        swap.wait_send()
    for move in moves:
        move.wait_send()
    for copy in copies:
        copy.wait_send()


def share_rows(lats, lons, table):
    rows = table.shape[0] // lons
    width = table.shape[1]
    zs = lons // 2
    sends = (zs - 1) + (lats - 1) + 1 + (zs - 1) * lats + zs * (lats - 1)
    dma = pltpu.SemaphoreType.DMA
    return pl.pallas_call(
        functools.partial(share_kernel, lats, lons),
        out_shape=jax.ShapeDtypeStruct((lats * lons, rows, width), jnp.bfloat16),
        in_specs=[pl.BlockSpec(memory_space=pltpu.VMEM), pl.BlockSpec(memory_space=pl.ANY)],
        out_specs=pl.BlockSpec(memory_space=pltpu.VMEM),
        scratch_shapes=[
            pltpu.VMEM((zs, rows, width), jnp.float32),
            pltpu.VMEM((zs, rows, width), jnp.float32),
            pltpu.VMEM((zs - 1, rows, width), jnp.float32),
            pltpu.VMEM((HIGH_BLOCKS * LANES, 2 * TILE), jnp.bfloat16),
            dma(()),
            dma((zs,)), dma((zs,)), dma((zs - 1,)), dma((zs - 1,)),
            dma((sends,)), dma((lats * lons,)),
        ],
        compiler_params=pltpu.CompilerParams(collective_id=0, has_side_effects=True),
        name="share_rows",
    )(table.reshape(lons, rows, width), jnp.asarray(running_sums()))


def body(lats, lons, transport, sigma_class, basin_id, depth_levels):
    table = bin_rows(transport, sigma_class, basin_id, depth_levels)
    whole = share_rows(lats, lons, table).reshape(-1, BASINS, TILE)
    return jnp.transpose(whole[:, :, :CLASSES], (1, 2, 0))


def solution(mesh):
    placed = (P(None, "lat", "lon"), P(None, "lat", "lon"), P("lat", "lon"), P("lat", "lon"))
    local = functools.partial(body, mesh.shape["lat"], mesh.shape["lon"])
    return jax.shard_map(local, mesh=mesh, in_specs=placed, out_specs=P(), check_vma=False)
```

```python
import functools

import jax
import jax.numpy as jnp
import numpy as np
from jax import lax
from jax.experimental import pallas as pl
from jax.experimental.pallas import tpu as pltpu
from jax.sharding import PartitionSpec as P

CLASSES = 200
BASINS = 4
SUB = 8
LANES = 128
TILE = 256
STEP_ROWS = 16
MESH = pl.DeviceIdType.MESH
HIGHS = 26
HIGH_BLOCKS = 4


def hot_pairs(index, count, value):
    return [jnp.where(index == jnp.bfloat16(2 * i), value, jnp.bfloat16(0)) for i in range(count)]


def doubled(index):
    pair = jnp.concatenate([index, index - 1], axis=0)
    return pair.astype(jnp.float32).astype(jnp.bfloat16)


def squeeze_rows(product):
    rows = lax.broadcasted_iota(jnp.int32, (SUB, TILE), 0)
    lanes = lax.broadcasted_iota(jnp.int32, (SUB, TILE), 1)
    own = (lanes % SUB) == rows
    blocks = []
    for q in range(HIGH_BLOCKS):
        total = None
        for s in range(SUB):
            high = q * SUB + s
            if high * SUB >= CLASSES:
                break
            piece = jnp.where(own, product[high * SUB:(high + 1) * SUB, :], 0.0)
            piece = piece if s == 0 else pltpu.roll(piece, s, 1)
            total = piece if total is None else total + piece
        straight = jnp.where(rows == 0, total, 0.0)
        for r in range(1, SUB):
            straight = jnp.where(rows == r, pltpu.roll(total, TILE - r, 1), straight)
        blocks.append(straight)
    return jnp.concatenate(blocks, axis=1)


def bin_block(flow_ref, class_ref, basin_ref, depth_ref, out_ref, *accs):
    levels, _, cols = class_ref.shape
    chunks = cols // LANES
    per_trip = 16
    for half in range(STEP_ROWS // SUB):
        rows = slice(half * SUB, (half + 1) * SUB)

        def trip(t, carry, rows=rows):
            tiles = []
            for u in range(per_trip):
                level = t * per_trip + u
                for c in range(chunks):
                    lanes = slice(c * LANES, (c + 1) * LANES)
                    klass = class_ref[level, rows, lanes]
                    flow = flow_ref[level, :, lanes].astype(jnp.float32)[rows]
                    flow = jnp.where(level < depth_ref[rows, lanes], flow, 0.0)
                    high = doubled(klass >> 3)
                    low = doubled(basin_ref[rows, lanes] * SUB + (klass & 7))
                    value = jnp.concatenate([flow, flow], axis=0).astype(jnp.bfloat16)
                    tiles.append((
                        jnp.concatenate(hot_pairs(high, HIGHS // 2, value), axis=0),
                        jnp.concatenate(hot_pairs(low, TILE // (2 * SUB), jnp.bfloat16(1)), axis=0),
                    ))
            for k in range(0, len(tiles), 2):
                mxu, stage = (k // 2) % 2, (k // 4) % 2
                left = jnp.concatenate([tiles[k][0], tiles[k + 1][0]], axis=1)
                right = jnp.concatenate([tiles[k][1], tiles[k + 1][1]], axis=1)
                pltpu.matmul_push_rhs(right, staging_register=stage, mxu_index=mxu, transpose=True)
                pltpu.matmul_acc_lhs(accs[mxu], left, load_staged_rhs=stage)
            return carry

        lax.fori_loop(0, levels // per_trip, trip, 0)
        product = pltpu.matmul_pop(accs[0]) + pltpu.matmul_pop(accs[1])
        out_ref[rows, :] = squeeze_rows(product)


def bin_kernel(*refs):
    shape = (HIGHS * SUB, TILE)
    pl.run_scoped(
        functools.partial(bin_block, *refs), *[pltpu.ACC(m)(shape, jnp.float32) for m in (0, 1)]
    )


def bin_rows(transport, sigma_class, basin_id, depth_levels):
    levels, row_count, cols = sigma_class.shape
    deep = pl.BlockSpec((levels, STEP_ROWS, cols), lambda i: (0, i, 0))
    flat = pl.BlockSpec((STEP_ROWS, cols), lambda i: (i, 0))
    width = HIGH_BLOCKS * TILE
    return pl.pallas_call(
        bin_kernel,
        grid=(row_count // STEP_ROWS,),
        in_specs=[deep, deep, flat, flat],
        out_specs=pl.BlockSpec((STEP_ROWS, width), lambda i: (i, 0)),
        out_shape=jax.ShapeDtypeStruct((row_count, width), jnp.float32),
        name="bin_rows",
    )(transport, sigma_class, basin_id, depth_levels)


def running_sums():
    row = np.arange(HIGH_BLOCKS * LANES)
    column = np.arange(2 * TILE)
    lane = row % LANES
    klass = (row // LANES) * 64 + (lane % SUB) * SUB + (lane % 64) // SUB
    same = (lane // 64)[:, None] == (column // TILE)[None, :]
    return (same & (klass[:, None] <= (column % TILE)[None, :])).astype(jnp.bfloat16)


def accumulate(share, sums):
    pieces = []
    for pair in range(BASINS // 2):
        lanes = [share[:, q * TILE + pair * LANES:q * TILE + (pair + 1) * LANES] for q in range(HIGH_BLOCKS)]
        rest = jnp.concatenate(lanes, axis=1)
        total = None
        for _ in range(3):
            part = rest.astype(jnp.bfloat16)
            rest = rest - part.astype(jnp.float32)
            term = jnp.dot(part, sums, preferred_element_type=jnp.float32)
            total = term if total is None else total + term
        pieces.append(total)
    return jnp.concatenate(pieces, axis=1)


def share_kernel(lats, lons, table_ref, sums_ref, out_ref, half, acc, arrived, sums, sum_sem,
                 half_send, half_recv, arr_send, arr_recv, out_send, out_recv):
    lat, lon = lax.axis_index("lat"), lax.axis_index("lon")
    zs = lons // 2
    z, core = lon // 2, lax.rem(lon, 2)
    partner = (lat, z * 2 + (1 - core))
    z_peers = [(lat, lax.rem(z + k, zs) * 2 + core) for k in range(1, zs)]
    lat_peers = [(lax.rem(lat + k, lats), lon) for k in range(1, lats)]

    load = pltpu.make_async_copy(sums_ref, sums, sum_sem)
    load.start()
    barrier = pltpu.get_barrier_semaphore()
    everyone = [partner] + z_peers + lat_peers
    for peer in everyone:
        pl.semaphore_signal(barrier, inc=1, device_id=peer, device_id_type=MESH)
    pl.semaphore_wait(barrier, len(everyone))

    def send(src, dst, send_sem, recv_sem, peer):
        copy = pltpu.make_async_remote_copy(
            src_ref=src, dst_ref=dst, send_sem=send_sem, recv_sem=recv_sem,
            device_id=peer, device_id_type=MESH,
        )
        copy.start()
        return copy

    swaps = []
    for k in [*range(1, zs), 0]:
        d = lax.rem(z + k, zs)
        swaps.append((k, send(table_ref.at[2 * d + (1 - core)], half.at[k], half_send.at[k], half_recv.at[k], partner)))
    moves = []
    for k, swap in swaps:
        swap.wait_recv()
        d = lax.rem(z + k, zs)
        acc[k] = table_ref[2 * d + core] + half[k]
        if k > 0:
            moves.append(send(acc.at[k], arrived.at[k - 1], arr_send.at[k - 1], arr_recv.at[k - 1], z_peers[k - 1]))
    share = acc[0]
    for k in range(1, zs):
        moves[k - 1].wait_recv()
        share = share + arrived[k - 1]
    load.wait()
    me = lat * lons + lon
    out_ref[me] = accumulate(share, sums[...]).astype(jnp.bfloat16)

    copies = []

    def spread(owner, peer):
        n = len(copies)
        copies.append(send(out_ref.at[owner], out_ref.at[owner], out_send.at[n], out_recv.at[owner], peer))

    def landed(owner):
        pltpu.make_async_remote_copy(
            src_ref=out_ref.at[owner], dst_ref=out_ref.at[owner], send_sem=out_send.at[0],
            recv_sem=out_recv.at[owner], device_id=partner, device_id_type=MESH,
        ).wait_recv()

    for peer in z_peers + lat_peers:
        spread(me, peer)
    spread(me, partner)
    for k in range(1, zs):
        owner = lat * lons + lax.rem(z - k + zs, zs) * 2 + core
        landed(owner)
        for peer in lat_peers + [partner]:
            spread(owner, peer)
    for j in range(zs):
        for k in range(1, lats):
            owner = lax.rem(lat - k + lats, lats) * lons + lax.rem(z - j + zs, zs) * 2 + core
            landed(owner)
            spread(owner, partner)
    for j in range(zs):
        for k in range(lats):
            landed(lax.rem(lat - k + lats, lats) * lons + lax.rem(z - j + zs, zs) * 2 + (1 - core))
    for _, swap in swaps:
        swap.wait_send()
    for move in moves:
        move.wait_send()
    for copy in copies:
        copy.wait_send()


def share_rows(lats, lons, table):
    rows = table.shape[0] // lons
    width = table.shape[1]
    zs = lons // 2
    sends = (zs - 1) + (lats - 1) + 1 + (zs - 1) * lats + zs * (lats - 1)
    dma = pltpu.SemaphoreType.DMA
    return pl.pallas_call(
        functools.partial(share_kernel, lats, lons),
        out_shape=jax.ShapeDtypeStruct((lats * lons, rows, width), jnp.bfloat16),
        in_specs=[pl.BlockSpec(memory_space=pltpu.VMEM), pl.BlockSpec(memory_space=pl.ANY)],
        out_specs=pl.BlockSpec(memory_space=pltpu.VMEM),
        scratch_shapes=[
            pltpu.VMEM((zs, rows, width), jnp.float32),
            pltpu.VMEM((zs, rows, width), jnp.float32),
            pltpu.VMEM((zs - 1, rows, width), jnp.float32),
            pltpu.VMEM((HIGH_BLOCKS * LANES, 2 * TILE), jnp.bfloat16),
            dma(()),
            dma((zs,)), dma((zs,)), dma((zs - 1,)), dma((zs - 1,)),
            dma((sends,)), dma((lats * lons,)),
        ],
        compiler_params=pltpu.CompilerParams(collective_id=0, has_side_effects=True),
        name="share_rows",
    )(table.reshape(lons, rows, width), jnp.asarray(running_sums()))


def body(lats, lons, transport, sigma_class, basin_id, depth_levels):
    table = bin_rows(transport, sigma_class, basin_id, depth_levels)
    whole = share_rows(lats, lons, table).reshape(-1, BASINS, TILE)
    return jnp.transpose(whole[:, :, :CLASSES], (1, 2, 0))


def solution(mesh):
    placed = (P(None, "lat", "lon"), P(None, "lat", "lon"), P("lat", "lon"), P("lat", "lon"))
    local = functools.partial(body, mesh.shape["lat"], mesh.shape["lon"])
    return jax.shard_map(local, mesh=mesh, in_specs=placed, out_specs=P(), check_vma=False)
```

```python
import functools

import jax
import jax.numpy as jnp
import numpy as np
from jax import lax
from jax.experimental import pallas as pl
from jax.experimental.pallas import tpu as pltpu
from jax.sharding import PartitionSpec as P

CLASSES = 200
BASINS = 4
SUB = 8
LANES = 128
TILE = 256
STEP_ROWS = 16
MESH = pl.DeviceIdType.MESH
HIGHS = 26
HIGH_BLOCKS = 4


def hot_pairs(index, count, value):
    return [jnp.where(index == jnp.bfloat16(2 * i), value, jnp.bfloat16(0)) for i in range(count)]


def doubled(index):
    pair = jnp.concatenate([index, index - 1], axis=0)
    return pair.astype(jnp.float32).astype(jnp.bfloat16)


def squeeze_rows(product):
    rows = lax.broadcasted_iota(jnp.int32, (SUB, TILE), 0)
    lanes = lax.broadcasted_iota(jnp.int32, (SUB, TILE), 1)
    own = (lanes % SUB) == rows
    blocks = []
    for q in range(HIGH_BLOCKS):
        total = None
        for s in range(SUB):
            high = q * SUB + s
            if high * SUB >= CLASSES:
                break
            piece = jnp.where(own, product[high * SUB:(high + 1) * SUB, :], 0.0)
            piece = piece if s == 0 else pltpu.roll(piece, s, 1)
            total = piece if total is None else total + piece
        straight = jnp.where(rows == 0, total, 0.0)
        for r in range(1, SUB):
            straight = jnp.where(rows == r, pltpu.roll(total, TILE - r, 1), straight)
        blocks.append(straight)
    return jnp.concatenate(blocks, axis=1)


def bin_block(flow_ref, class_ref, basin_ref, depth_ref, out_ref, *accs):
    levels, _, cols = class_ref.shape
    chunks = cols // LANES
    per_trip = 24
    for half in range(STEP_ROWS // SUB):
        rows = slice(half * SUB, (half + 1) * SUB)

        def trip(t, carry, rows=rows):
            tiles = []
            for u in range(per_trip):
                level = t * per_trip + u
                for c in range(chunks):
                    lanes = slice(c * LANES, (c + 1) * LANES)
                    klass = class_ref[level, rows, lanes]
                    flow = flow_ref[level, :, lanes].astype(jnp.float32)[rows]
                    flow = jnp.where(level < depth_ref[rows, lanes], flow, 0.0)
                    high = doubled(klass >> 3)
                    low = doubled(basin_ref[rows, lanes] * SUB + (klass & 7))
                    value = jnp.concatenate([flow, flow], axis=0).astype(jnp.bfloat16)
                    tiles.append((
                        jnp.concatenate(hot_pairs(high, HIGHS // 2, value), axis=0),
                        jnp.concatenate(hot_pairs(low, TILE // (2 * SUB), jnp.bfloat16(1)), axis=0),
                    ))
            for k in range(0, len(tiles), 2):
                mxu, stage = (k // 2) % 2, (k // 4) % 2
                left = jnp.concatenate([tiles[k][0], tiles[k + 1][0]], axis=1)
                right = jnp.concatenate([tiles[k][1], tiles[k + 1][1]], axis=1)
                pltpu.matmul_push_rhs(right, staging_register=stage, mxu_index=mxu, transpose=True)
                pltpu.matmul_acc_lhs(accs[mxu], left, load_staged_rhs=stage)
            return carry

        lax.fori_loop(0, levels // per_trip, trip, 0)
        product = pltpu.matmul_pop(accs[0]) + pltpu.matmul_pop(accs[1])
        out_ref[rows, :] = squeeze_rows(product)


def bin_kernel(*refs):
    shape = (HIGHS * SUB, TILE)
    pl.run_scoped(
        functools.partial(bin_block, *refs), *[pltpu.ACC(m)(shape, jnp.float32) for m in (0, 1)]
    )


def bin_rows(transport, sigma_class, basin_id, depth_levels):
    levels, row_count, cols = sigma_class.shape
    deep = pl.BlockSpec((levels, STEP_ROWS, cols), lambda i: (0, i, 0))
    flat = pl.BlockSpec((STEP_ROWS, cols), lambda i: (i, 0))
    width = HIGH_BLOCKS * TILE
    return pl.pallas_call(
        bin_kernel,
        grid=(row_count // STEP_ROWS,),
        in_specs=[deep, deep, flat, flat],
        out_specs=pl.BlockSpec((STEP_ROWS, width), lambda i: (i, 0)),
        out_shape=jax.ShapeDtypeStruct((row_count, width), jnp.float32),
        name="bin_rows",
    )(transport, sigma_class, basin_id, depth_levels)


def running_sums():
    row = np.arange(HIGH_BLOCKS * LANES)
    column = np.arange(2 * TILE)
    lane = row % LANES
    klass = (row // LANES) * 64 + (lane % SUB) * SUB + (lane % 64) // SUB
    same = (lane // 64)[:, None] == (column // TILE)[None, :]
    return (same & (klass[:, None] <= (column % TILE)[None, :])).astype(jnp.bfloat16)


def accumulate(share, sums):
    pieces = []
    for pair in range(BASINS // 2):
        lanes = [share[:, q * TILE + pair * LANES:q * TILE + (pair + 1) * LANES] for q in range(HIGH_BLOCKS)]
        rest = jnp.concatenate(lanes, axis=1)
        total = None
        for _ in range(3):
            part = rest.astype(jnp.bfloat16)
            rest = rest - part.astype(jnp.float32)
            term = jnp.dot(part, sums, preferred_element_type=jnp.float32)
            total = term if total is None else total + term
        pieces.append(total)
    return jnp.concatenate(pieces, axis=1)


def share_kernel(lats, lons, table_ref, sums_ref, out_ref, half, acc, arrived, sums, sum_sem,
                 half_send, half_recv, arr_send, arr_recv, out_send, out_recv):
    lat, lon = lax.axis_index("lat"), lax.axis_index("lon")
    zs = lons // 2
    z, core = lon // 2, lax.rem(lon, 2)
    partner = (lat, z * 2 + (1 - core))
    z_peers = [(lat, lax.rem(z + k, zs) * 2 + core) for k in range(1, zs)]
    lat_peers = [(lax.rem(lat + k, lats), lon) for k in range(1, lats)]

    load = pltpu.make_async_copy(sums_ref, sums, sum_sem)
    load.start()
    barrier = pltpu.get_barrier_semaphore()
    everyone = [partner] + z_peers + lat_peers
    for peer in everyone:
        pl.semaphore_signal(barrier, inc=1, device_id=peer, device_id_type=MESH)
    pl.semaphore_wait(barrier, len(everyone))

    def send(src, dst, send_sem, recv_sem, peer):
        copy = pltpu.make_async_remote_copy(
            src_ref=src, dst_ref=dst, send_sem=send_sem, recv_sem=recv_sem,
            device_id=peer, device_id_type=MESH,
        )
        copy.start()
        return copy

    swaps = []
    for k in [*range(1, zs), 0]:
        d = lax.rem(z + k, zs)
        swaps.append((k, send(table_ref.at[2 * d + (1 - core)], half.at[k], half_send.at[k], half_recv.at[k], partner)))
    moves = []
    for k, swap in swaps:
        swap.wait_recv()
        d = lax.rem(z + k, zs)
        acc[k] = table_ref[2 * d + core] + half[k]
        if k > 0:
            moves.append(send(acc.at[k], arrived.at[k - 1], arr_send.at[k - 1], arr_recv.at[k - 1], z_peers[k - 1]))
    share = acc[0]
    for k in range(1, zs):
        moves[k - 1].wait_recv()
        share = share + arrived[k - 1]
    load.wait()
    me = lat * lons + lon
    out_ref[me] = accumulate(share, sums[...]).astype(jnp.bfloat16)

    copies = []

    def spread(owner, peer):
        n = len(copies)
        copies.append(send(out_ref.at[owner], out_ref.at[owner], out_send.at[n], out_recv.at[owner], peer))

    def landed(owner):
        pltpu.make_async_remote_copy(
            src_ref=out_ref.at[owner], dst_ref=out_ref.at[owner], send_sem=out_send.at[0],
            recv_sem=out_recv.at[owner], device_id=partner, device_id_type=MESH,
        ).wait_recv()

    for peer in z_peers + lat_peers:
        spread(me, peer)
    spread(me, partner)
    for k in range(1, zs):
        owner = lat * lons + lax.rem(z - k + zs, zs) * 2 + core
        landed(owner)
        for peer in lat_peers + [partner]:
            spread(owner, peer)
    for j in range(zs):
        for k in range(1, lats):
            owner = lax.rem(lat - k + lats, lats) * lons + lax.rem(z - j + zs, zs) * 2 + core
            landed(owner)
            spread(owner, partner)
    for j in range(zs):
        for k in range(lats):
            landed(lax.rem(lat - k + lats, lats) * lons + lax.rem(z - j + zs, zs) * 2 + (1 - core))
    for _, swap in swaps:
        swap.wait_send()
    for move in moves:
        move.wait_send()
    for copy in copies:
        copy.wait_send()


def share_rows(lats, lons, table):
    rows = table.shape[0] // lons
    width = table.shape[1]
    zs = lons // 2
    sends = (zs - 1) + (lats - 1) + 1 + (zs - 1) * lats + zs * (lats - 1)
    dma = pltpu.SemaphoreType.DMA
    return pl.pallas_call(
        functools.partial(share_kernel, lats, lons),
        out_shape=jax.ShapeDtypeStruct((lats * lons, rows, width), jnp.bfloat16),
        in_specs=[pl.BlockSpec(memory_space=pltpu.VMEM), pl.BlockSpec(memory_space=pl.ANY)],
        out_specs=pl.BlockSpec(memory_space=pltpu.VMEM),
        scratch_shapes=[
            pltpu.VMEM((zs, rows, width), jnp.float32),
            pltpu.VMEM((zs, rows, width), jnp.float32),
            pltpu.VMEM((zs - 1, rows, width), jnp.float32),
            pltpu.VMEM((HIGH_BLOCKS * LANES, 2 * TILE), jnp.bfloat16),
            dma(()),
            dma((zs,)), dma((zs,)), dma((zs - 1,)), dma((zs - 1,)),
            dma((sends,)), dma((lats * lons,)),
        ],
        compiler_params=pltpu.CompilerParams(collective_id=0, has_side_effects=True),
        name="share_rows",
    )(table.reshape(lons, rows, width), jnp.asarray(running_sums()))


def body(lats, lons, transport, sigma_class, basin_id, depth_levels):
    table = bin_rows(transport, sigma_class, basin_id, depth_levels)
    whole = share_rows(lats, lons, table).reshape(-1, BASINS, TILE)
    return jnp.transpose(whole[:, :, :CLASSES], (1, 2, 0))


def solution(mesh):
    placed = (P(None, "lat", "lon"), P(None, "lat", "lon"), P("lat", "lon"), P("lat", "lon"))
    local = functools.partial(body, mesh.shape["lat"], mesh.shape["lon"])
    return jax.shard_map(local, mesh=mesh, in_specs=placed, out_specs=P(), check_vma=False)
```
